1024 devices in a mesh: tile: 64 (over z, x), conv: 16 (over y, core).
Axes of the slice: x: 8, y: 8, z: 8, core: 2. Of those that a mesh axis runs over, the one named last changes fastest.
Arguments:
- field: float32 [256, 786432], P(None, ('tile', 'conv')), may hold values from -6 to 6
- interp: bfloat16 [1048576, 384], P(('tile', 'conv')), may hold values from -0.1875 to 0.1875
- conv_blocks: bfloat16 [2048, 3, 256, 256], P(('tile', 'conv')), may hold values from -0.21875 to 0.21875
- band_shift: int32 [2048, 3], P(('tile', 'conv')), may hold values from 0 to 1
- owner: int32 [393216, 1], P(('tile', 'conv')), may hold values from 0 to 15; in each aligned block of 384 rows (0 to 383, 384 to 767, ...) at most 32 rows name the same one
- edge_index: int32 [2048, 128], P(('tile', 'conv')), may hold values from 0 to 767, as said below
Outputs:
- correlated: float32 [256, 786432], P(None, ('tile', 'conv'))
The draws below stay inside these ranges and needn't reach their ends.
Inputs may be any that keep to these rules, and one draw needn't show every extreme that they name: `edge_index`: row 2b lists the first 128 columns of domain b in some order, row 2b + 1 its last 128 columns in some order. Among the 384 points of one domain no owner is named more than 32 times, and in some domains one owner is named exactly 32 times.
All inputs are finite; a program needn't handle non-finite values.
Results may differ from the reference program's by a relative error of at most 0.0049.
Values may be sent and summed in bfloat16 or wider, within the bound.
A program may use at most 32 MiB of HBM per device.

```python
import math
import jax
import jax.numpy as jnp
import numpy as np
from jax import lax

COLUMNS = 768
HALO_WIDTH = 128
BLOCK_POINTS = 256
OWNER_BLOCKS = 2
BAND_COUNT = 3
FIELD_ROWS = 256
DOMAINS = 1024
ALL_COLUMNS = 786432
EXTENDED = 1024
SLOTS = 512
SUBPOINTS = 384
CAPACITY = 32
ALL_SUBPOINTS = 393216
N_TILE = 64
N_CONV = 16


def draw_edge_index(key, part):
    row_keys = jax.random.split(key, 2 * DOMAINS)
    orders = jax.vmap(lambda single: jax.random.permutation(single, HALO_WIDTH))(row_keys)
    side_flags = jnp.arange(2 * DOMAINS, dtype=jnp.int32) % 2
    offsets = side_flags * (COLUMNS - HALO_WIDTH)
    return (orders.astype(jnp.int32) + offsets[:, None]).astype(jnp.int32)


def with_ends(values, own_key, smallest, high):
    longest = values.shape.index(max(values.shape))
    spots = []
    for shift in (0, 1):
        where = [jax.random.randint(jax.random.fold_in(own_key, axis), (), 0, length) for axis, length in enumerate(values.shape)]
        where[longest] = (where[longest] + shift) % values.shape[longest]
        spots.append(tuple(where))
    return values.at[spots[0]].set(smallest).at[spots[1]].set(high)


def steps_of(key, shape, cuts, low, top_value):
    gain, own = 1.0, jax.random.fold_in(key, 6)
    for axis_at, shards_of in cuts:
        steps = jnp.exp(jax.random.uniform(jax.random.fold_in(own, axis_at), (shards_of,), jnp.float32, low / len(cuts), top_value / len(cuts)))
        gain = gain * jnp.repeat(steps, shape[axis_at] // shards_of).reshape([-1 if axis == axis_at else 1 for axis in range(len(shape))])
    return gain


def routed_block(own_key, own, number, rows, amount, top, limit, skew):
    sequence = jax.random.permutation(own_key, amount)
    crowded, ordinary = portions_of(amount, rows * top, limit, skew, True), portions_of(amount, rows * top, limit, skew, False)
    places = jnp.arange(amount)

    def named(sizes, rotation):
        used = int((sizes > 0).sum())
        fixed = max(1, used // 4)
        passed = fixed + (places - fixed + rotation * (used - fixed)) % max(1, amount - fixed)
        return jnp.zeros((amount,), jnp.int32).at[sequence[jnp.where(places < fixed, places, passed)]].set(jnp.asarray(sizes, jnp.int32))

    sizes = jnp.where(number % 4 == 0, named(crowded, number // 4), named(ordinary, number - number // 4 - 1))
    mixed = jax.random.permutation(jax.random.fold_in(own, 3), amount)
    source_of, taker = mixed[0:amount // 2 * 2:2], mixed[1:amount // 2 * 2:2]
    room = jnp.minimum(sizes[source_of] - 1, limit - sizes[taker]) // 2
    room = jnp.where((source_of == sequence[0]) | (taker == sequence[0]) | (sizes[taker] == 0), 0, jnp.maximum(room, 0))
    passed = jax.random.randint(jax.random.fold_in(own, 4), (amount // 2,), 0, 1 << 20) % (room + 1)
    sizes = sizes.at[source_of].add(-passed).at[taker].add(passed)
    members = jnp.searchsorted(jnp.cumsum(sizes), jnp.arange(rows * top), side="right").astype(jnp.int32)
    listing = members.reshape(top, rows).T
    listing = listing[jax.random.permutation(jax.random.fold_in(own, 1), rows)]
    rotation = jax.random.randint(jax.random.fold_in(own, 2), (rows, 1), 0, top)
    return jnp.take_along_axis(listing, (jnp.arange(top)[None, :] + rotation) % top, axis=1)


def portions_of(count, total, reach, slope, full):
    loads = [(1 << 20) // math.isqrt(grade ** slope) + 1 for grade in range(1, count + 1)]
    largest = reach if full else min(reach, max(-(-total // count), total * loads[0] // sum(loads)))
    least = 1 if total - largest >= count - 1 else 0
    holding, surplus = [largest] + [least] * (count - 1), total - largest - least * (count - 1)
    while surplus > 0:
        movable = [i for i in range(1, count) if holding[i] < largest] or [i for i in range(1, count) if holding[i] < reach]
        mass, remaining = sum([loads[i] for i in movable]), surplus
        for i in movable:
            addition = min(reach - holding[i], max(1, remaining * loads[i] // mass), surplus)
            holding[i] = holding[i] + addition
            surplus = surplus - addition
    return np.array(holding)


def gaussian(stream_key, dims, width, limit, cuts=(), kind=jnp.bfloat16):
    drawn = width * jax.random.normal(stream_key, dims, jnp.float32)
    if cuts:
        drawn = drawn * steps_of(stream_key, dims, cuts, -0.22, 0.18)
    return jnp.clip(drawn, -limit, limit).astype(kind)


def setup_inputs(seed: int = 0) -> dict:
    streams_of = jax.random.split(jax.random.key(seed), 7)
    field = gaussian(streams_of[0], (FIELD_ROWS, ALL_COLUMNS), 1.0, 6.0, ((1, 1024),), jnp.float32)
    interp = gaussian(streams_of[1], (DOMAINS * EXTENDED, SUBPOINTS), EXTENDED ** -0.5, 0.1875, ((0, 1024),))
    conv_blocks = gaussian(streams_of[2], (DOMAINS * OWNER_BLOCKS, BAND_COUNT, BLOCK_POINTS, BLOCK_POINTS), (BAND_COUNT * BLOCK_POINTS) ** -0.5, 0.21875, ((0, 1024),))
    band_shift = with_ends(jax.random.randint(streams_of[3], (DOMAINS * OWNER_BLOCKS, BAND_COUNT), 0, OWNER_BLOCKS), jax.random.fold_in(streams_of[3], 1), 0, OWNER_BLOCKS - 1).astype(jnp.int32)
    owner_keys = jax.random.split(jax.random.fold_in(streams_of[4], 1), ALL_SUBPOINTS // SUBPOINTS)
    owner_turns = jax.random.permutation(jax.random.fold_in(streams_of[4], 3), ALL_SUBPOINTS // SUBPOINTS)
    owner = jax.vmap(lambda own, number: routed_block(jax.random.fold_in(streams_of[4], 2), own, number, SUBPOINTS, N_CONV, 1, CAPACITY, 2))(owner_keys, owner_turns).reshape((ALL_SUBPOINTS, 1))
    edge_index = draw_edge_index(jax.random.fold_in(streams_of[6], 71), 0)
    return dict(field=field, interp=interp, conv_blocks=conv_blocks, band_shift=band_shift, owner=owner, edge_index=edge_index)


def slot_table(owners):
    choose = (owners[:, None] == jnp.arange(N_CONV, dtype=jnp.int32)[None, :]).astype(jnp.int32)
    before = jnp.cumsum(choose, axis=0) - choose
    position = jnp.sum(before * choose, axis=1)
    slot_index = owners * CAPACITY + position
    return (slot_index[:, None] == jnp.arange(SLOTS, dtype=jnp.int32)[None, :]).astype(jnp.float32)


def interpolate(operands):
    extended, weights, owners = operands
    subgrid = jnp.dot(extended, weights, preferred_element_type=jnp.float32).astype(jnp.bfloat16)
    packed = jnp.dot(subgrid.astype(jnp.float32), slot_table(owners), precision=lax.Precision.HIGHEST)
    return packed.astype(jnp.bfloat16)


def convolve(operands):
    values, blocks, shifts = operands
    height = values.shape[0]
    pieces = values.reshape(height, OWNER_BLOCKS, BLOCK_POINTS).astype(jnp.float32)
    source = (jnp.arange(OWNER_BLOCKS, dtype=jnp.int32)[:, None] + shifts) % OWNER_BLOCKS
    picked = pieces[:, source, :]
    matrices = blocks.astype(jnp.float32)
    forward = jnp.einsum("rjbp,jbpq->rjq", picked, matrices, precision=lax.Precision.HIGHEST).astype(jnp.bfloat16)
    backward = jnp.einsum("rjq,jbpq->rjbp", forward.astype(jnp.float32), matrices, precision=lax.Precision.HIGHEST)
    select = (source[:, :, None] == jnp.arange(OWNER_BLOCKS, dtype=jnp.int32)[None, None, :]).astype(jnp.float32)
    adjoint = jnp.einsum("rjbp,jbs->rsp", backward, select, precision=lax.Precision.HIGHEST)
    return adjoint.reshape(height, SLOTS).astype(jnp.bfloat16)


def adjoint_interpolate(operands):
    returned_slots, weights, owners = operands
    returned = jnp.dot(returned_slots.astype(jnp.float32), slot_table(owners).T, precision=lax.Precision.HIGHEST)
    returned = returned.astype(jnp.bfloat16)
    return jnp.dot(returned, weights.T, preferred_element_type=jnp.float32)


def add_edges(inner_part, left_sum, right_sum, left_list, right_list):
    inner_part = inner_part.at[:, left_list].add(left_sum)
    return inner_part.at[:, right_list].add(right_sum)


def reference(field, interp, conv_blocks, band_shift, owner, edge_index):
    field_rows = field.shape[0]
    rounded = field.astype(jnp.bfloat16).reshape(field_rows, DOMAINS, COLUMNS).transpose(1, 0, 2)
    edges = edge_index.reshape(DOMAINS, 2, HALO_WIDTH)
    left_lists = edges[:, 0, :]
    right_lists = edges[:, 1, :]
    left_index = jnp.broadcast_to(left_lists[:, None, :], (DOMAINS, field_rows, HALO_WIDTH))
    right_index = jnp.broadcast_to(right_lists[:, None, :], (DOMAINS, field_rows, HALO_WIDTH))
    left_values = jnp.take_along_axis(rounded, left_index, axis=2)
    right_values = jnp.take_along_axis(rounded, right_index, axis=2)
    extended = jnp.concatenate([jnp.roll(right_values, 1, axis=0), rounded, jnp.roll(left_values, -1, axis=0)], axis=2)
    weights = interp.reshape(DOMAINS, EXTENDED, SUBPOINTS)
    owners = owner.reshape(DOMAINS, SUBPOINTS)
    packed = lax.map(interpolate, (extended, weights, owners))
    gathered = packed.reshape(N_TILE, N_CONV, field_rows, N_CONV, CAPACITY).transpose(0, 3, 2, 1, 4)
    gathered = gathered.reshape(DOMAINS, field_rows, SLOTS)
    blocks = conv_blocks.reshape(DOMAINS, OWNER_BLOCKS, BAND_COUNT, BLOCK_POINTS, BLOCK_POINTS)
    shifts = band_shift.reshape(DOMAINS, OWNER_BLOCKS, BAND_COUNT)
    adjoints = lax.map(convolve, (gathered, blocks, shifts))
    returned = adjoints.reshape(N_TILE, N_CONV, field_rows, N_CONV, CAPACITY).transpose(0, 3, 2, 1, 4)
    returned = returned.reshape(DOMAINS, field_rows, SLOTS)
    partial_value = lax.map(adjoint_interpolate, (returned, weights, owners))
    interior = partial_value[:, :, HALO_WIDTH:HALO_WIDTH + COLUMNS]
    left_sums = jnp.roll(partial_value[:, :, HALO_WIDTH + COLUMNS:], 1, axis=0)
    right_sums = jnp.roll(partial_value[:, :, :HALO_WIDTH], -1, axis=0)
    result = jax.vmap(add_edges)(interior, left_sums, right_sums, left_lists, right_lists)
    return result.transpose(1, 0, 2).reshape(field_rows, DOMAINS * COLUMNS)
```

```python
import jax
import jax.numpy as jnp
from jax import lax
from jax.experimental import pallas as pl
from jax.experimental.pallas import tpu as pltpu
from jax.sharding import PartitionSpec as P

MESH = pl.DeviceIdType.MESH
F32 = jnp.float32
BF16 = jnp.bfloat16
NT = (((1,), (1,)), ((), ()))
NN = (((1,), (0,)), ((), ()))


def mm(a, b, dims=NN):
    return lax.dot_general(a, b, dims, preferred_element_type=F32)


def make_kernel(n_tile, n_conv, rows, columns, rim, points, blocks, bands, block_points):
    slots = blocks * block_points
    cap = slots // n_conv
    per_block = block_points // cap
    half = 128
    halves = rows // half
    offsets = sorted(range(1, n_conv), key=lambda d: (-min(d, n_conv - d), d))

    def kernel(
        field, interp, conv, shift, owner, edges, out,
        xf, ib, wb, sh, ow, eg, rims, halo, pt, qt, xb, mid, out_t, g_t0, g_t1, adj_t, inc_t, edge_out, edge_in, wt,
        load_sem, halo_send, halo_recv, go_send, go_recv, back_send, back_recv, edge_send, edge_recv,
    ):
        tile = lax.axis_index("tile")
        me = lax.axis_index("conv")
        index = tile * n_conv + me
        total = n_tile * n_conv
        right = lax.rem(index + 1, total)
        left = lax.rem(index + total - 1, total)
        right_id = (right // n_conv, lax.rem(right, n_conv))
        left_id = (left // n_conv, lax.rem(left, n_conv))

        def peer(d):
            return (tile, lax.rem(me + d, n_conv))

        barrier = pltpu.get_barrier_semaphore()
        for target in [left_id, right_id] + [peer(d) for d in offsets]:
            pl.semaphore_signal(barrier, inc=1, device_id=target, device_id_type=MESH)

        loads = [
            pltpu.make_async_copy(edges, eg, load_sem.at[0]),
            pltpu.make_async_copy(field.at[:, pl.ds(columns - rim, rim)], xf.at[:, pl.ds(columns - rim, rim)], load_sem.at[1]),
            pltpu.make_async_copy(field.at[:, pl.ds(0, rim)], xf.at[:, pl.ds(0, rim)], load_sem.at[2]),
            pltpu.make_async_copy(owner, ow, load_sem.at[3]),
            pltpu.make_async_copy(interp, ib, load_sem.at[4]),
            pltpu.make_async_copy(
                field.at[:, pl.ds(rim, columns - 2 * rim)], xf.at[:, pl.ds(rim, columns - 2 * rim)], load_sem.at[5]
            ),
            pltpu.make_async_copy(conv, wb, load_sem.at[6]),
            pltpu.make_async_copy(shift, sh, load_sem.at[7]),
        ]
        for load in loads:
            load.start()

        for i in range(3):
            loads[i].wait()
        down = lax.broadcasted_iota(jnp.int32, (rim, rim), 0)
        pick_left = (down == eg[0:1, :]).astype(F32).astype(BF16)
        pick_right = (down + (columns - rim) == eg[1:2, :]).astype(F32).astype(BF16)
        edge_cols = (slice(columns - rim, columns), slice(0, rim))
        for side, pick in ((0, pick_right), (1, pick_left)):
            cells = xf[:, edge_cols[side]].astype(BF16)
            xb[:, edge_cols[side]] = cells
            rims[side] = mm(cells, pick).astype(BF16).reshape(halves, half, rim)

        pl.semaphore_wait(barrier, n_conv + 1)

        halo_copies = []
        for h in range(halves):
            for side, target in ((0, right_id), (1, left_id)):
                copy = pltpu.make_async_remote_copy(
                    src_ref=rims.at[side, h], dst_ref=halo.at[side, h],
                    send_sem=halo_send.at[side, h], recv_sem=halo_recv.at[side, h],
                    device_id=target, device_id_type=MESH,
                )
                copy.start()
                halo_copies.append(copy)

        loads[3].wait()
        owners = ow[...]
        named = (lax.broadcasted_iota(jnp.int32, (n_conv, points), 0) == owners).astype(F32)
        earlier = (
            lax.broadcasted_iota(jnp.int32, (points, points), 0) < lax.broadcasted_iota(jnp.int32, (points, points), 1)
        ).astype(F32).astype(BF16)
        before = mm(named.astype(BF16), earlier)
        rank = jnp.sum(before * named, axis=0, keepdims=True)
        slot = owners.astype(F32) * cap + rank
        pt[...] = (lax.broadcasted_iota(jnp.int32, (slots, points), 0).astype(F32) == slot).astype(F32).astype(BF16)
        loads[4].wait()
        extended = columns + 2 * rim
        for start in range(0, extended, 256):
            qt[:, start:start + 256] = mm(pt[...], ib[start:start + 256, :], NT).astype(BF16)
        loads[5].wait()
        xb[:, rim:columns - rim] = xf[:, rim:columns - rim].astype(BF16)
        for h in range(halves):
            mid[h] = mm(qt[:, rim:rim + columns], xb[h * half:(h + 1) * half, :], NT)

        g_t = (g_t0, g_t1)
        inc = (inc_t.at[0], inc_t.at[1])

        def exchange(h, src, dst, send, recv):
            copies = []
            for d in offsets:
                to = lax.rem(me + d, n_conv)
                copy = pltpu.make_async_remote_copy(
                    src_ref=src.at[h, to // per_block, pl.ds(pl.multiple_of(lax.rem(to, per_block) * cap, cap), cap)],
                    dst_ref=dst.at[me // per_block, pl.ds(pl.multiple_of(lax.rem(me, per_block) * cap, cap), cap)],
                    send_sem=send.at[h, d], recv_sem=recv.at[h, d],
                    device_id=peer(d), device_id_type=MESH,
                )
                copy.start()
                copies.append(copy)
            mine = pl.ds(pl.multiple_of(lax.rem(me, per_block) * cap, cap), cap)
            dst[me // per_block, mine, :] = src[h, me // per_block, mine, :]
            return copies

        going = []
        for h in range(halves):
            halo_copies[2 * h].wait_recv()
            halo_copies[2 * h + 1].wait_recv()
            sub = mid[h] + mm(qt[:, 0:rim], halo[0, h], NT) + mm(qt[:, rim + columns:], halo[1, h], NT)
            out_t[h] = sub.astype(BF16).reshape(blocks, block_points, half)
            going.append(exchange(h, out_t, g_t[h], go_send, go_recv))

        loads[6].wait()
        loads[7].wait()
        for j in range(blocks):
            for c in range(bands):
                wt[j, :, c * block_points:(c + 1) * block_points] = wb[j, c].T

        coming = []
        for h in range(halves):
            for copy in going[h]:
                copy.wait_recv()
            sums = [None] * blocks
            for j in range(blocks):
                sources = [lax.rem(sh[j, c] + j, blocks) for c in range(bands)]
                picked = jnp.concatenate([g_t[h][s] for s in sources], axis=0)
                forward = mm(wt[j], picked).astype(BF16)
                for c in range(bands):
                    term = mm(wb[j, c], forward)
                    for s in range(blocks):
                        part = term * (sources[c] == s).astype(F32)
                        sums[s] = part if sums[s] is None else sums[s] + part
            for s in range(blocks):
                adj_t[h, s] = sums[s].astype(BF16)
            coming.append(exchange(h, adj_t, inc[h], back_send, back_recv))

        edge_copies = []
        for h in range(halves):
            for copy in coming[h]:
                copy.wait_recv()
            came = inc_t[h].reshape(slots, half).T
            edge_out[0, h] = mm(came, qt[:, rim + columns:]).astype(BF16)
            edge_out[1, h] = mm(came, qt[:, 0:rim]).astype(BF16)
            for side, target in ((0, right_id), (1, left_id)):
                copy = pltpu.make_async_remote_copy(
                    src_ref=edge_out.at[side, h], dst_ref=edge_in.at[side, h],
                    send_sem=edge_send.at[side, h], recv_sem=edge_recv.at[side, h],
                    device_id=target, device_id_type=MESH,
                )
                copy.start()
                edge_copies.append(copy)
            out[h * half:(h + 1) * half, :] = mm(came, qt[:, rim:rim + columns])
        for h in range(halves):
            span = slice(h * half, (h + 1) * half)
            edge_copies[2 * h].wait_recv()
            edge_copies[2 * h + 1].wait_recv()
            out[span, 0:rim] += mm(edge_in[0, h], pick_left, NT)
            out[span, columns - rim:columns] += mm(edge_in[1, h], pick_right, NT)
        for copy in halo_copies + sum(going, []) + sum(coming, []) + edge_copies:
            copy.wait_send()

    return kernel


def solution(mesh):
    n_tile, n_conv = mesh.shape["tile"], mesh.shape["conv"]

    def on_device(field, interp, conv_blocks, band_shift, owner, edge_index):
        rows, columns = field.shape
        rim = edge_index.shape[1]
        extended, points = interp.shape
        blocks, bands, block_points, _ = conv_blocks.shape
        slots = blocks * block_points
        half, halves = 128, rows // 128
        body = make_kernel(n_tile, n_conv, rows, columns, rim, points, blocks, bands, block_points)
        sides = (2, halves, half, rim)
        cells = (halves, blocks, block_points, half)
        operands = [
            pltpu.with_memory_space_constraint(x, pltpu.HBM)
            for x in (field, interp, conv_blocks, band_shift, owner.reshape(1, points), edge_index)
        ]
        return pl.pallas_call(
            body,
            out_shape=jax.ShapeDtypeStruct((rows, columns), F32),
            in_specs=[pl.BlockSpec(memory_space=pltpu.HBM)] * 6,
            out_specs=pl.BlockSpec(memory_space=pltpu.VMEM),
            scratch_shapes=[
                pltpu.VMEM((rows, columns), F32),
                pltpu.VMEM((extended, points), BF16),
                pltpu.VMEM((blocks, bands, block_points, block_points), BF16),
                pltpu.SMEM((blocks, bands), jnp.int32),
                pltpu.VMEM((1, points), jnp.int32),
                pltpu.VMEM((2, rim), jnp.int32),
                pltpu.VMEM(sides, BF16),
                pltpu.VMEM(sides, BF16),
                pltpu.VMEM((slots, points), BF16),
                pltpu.VMEM((slots, extended), BF16),
                pltpu.VMEM((rows, columns), BF16),
                pltpu.VMEM((halves, slots, half), F32),
                pltpu.VMEM(cells, BF16),
                pltpu.VMEM(cells[1:], BF16),
                pltpu.VMEM(cells[1:], BF16),
                pltpu.VMEM(cells, BF16),
                pltpu.VMEM(cells, BF16),
                pltpu.VMEM(sides, BF16),
                pltpu.VMEM(sides, BF16),
                pltpu.VMEM((blocks, block_points, bands * block_points), BF16),
                pltpu.SemaphoreType.DMA((8,)),
                pltpu.SemaphoreType.DMA((2, halves)),
                pltpu.SemaphoreType.DMA((2, halves)),
                pltpu.SemaphoreType.DMA((halves, n_conv)),
                pltpu.SemaphoreType.DMA((halves, n_conv)),
                pltpu.SemaphoreType.DMA((halves, n_conv)),
                pltpu.SemaphoreType.DMA((halves, n_conv)),
                pltpu.SemaphoreType.DMA((2, halves)),
                pltpu.SemaphoreType.DMA((2, halves)),
            ],
            compiler_params=pltpu.CompilerParams(
                collective_id=0, has_side_effects=True, vmem_limit_bytes=24 * 1024 * 1024
            ),
        )(*operands)

    return jax.shard_map(
        on_device,
        mesh=mesh,
        in_specs=(
            P(None, ("tile", "conv")),
            P(("tile", "conv"), None),
            P(("tile", "conv"), None, None, None),
            P(("tile", "conv"), None),
            P(("tile", "conv"), None),
            P(("tile", "conv"), None),
        ),
        out_specs=P(None, ("tile", "conv")),
        check_vma=False,
    )
```

```python
import jax
import jax.numpy as jnp
from jax import lax
from jax.experimental import pallas as pl
from jax.experimental.pallas import tpu as pltpu
from jax.sharding import PartitionSpec as P

MESH = pl.DeviceIdType.MESH
F32 = jnp.float32
BF16 = jnp.bfloat16
NT = (((1,), (1,)), ((), ()))
NN = (((1,), (0,)), ((), ()))


def mm(a, b, dims=NN):
    return lax.dot_general(a, b, dims, preferred_element_type=F32)


def choose(pieces, source):
    chosen = pieces[0]
    for s in range(1, len(pieces)):
        chosen = jnp.where(source == s, pieces[s], chosen)
    return chosen


def make_kernel(n_tile, n_conv, rows, columns, rim, points, blocks, bands, block_points):
    slots = blocks * block_points
    cap = slots // n_conv
    half = 128
    halves = rows // half
    offsets = sorted(range(1, n_conv), key=lambda d: (-min(d, n_conv - d), d))

    def kernel(
        field, interp, conv, shift, owner, edges, out,
        xf, ib, wb, sh, ow, eg, rims, halo, pt, qt, xb, mid, out_t, g_t0, g_t1, adj_t, inc_t, edge_out, edge_in, wt,
        load_sem, halo_send, halo_recv, go_send, go_recv, back_send, back_recv, edge_send, edge_recv,
        near, up, down_sem,
    ):
        tile = lax.axis_index("tile")
        me = lax.axis_index("conv")
        index = tile * n_conv + me
        total = n_tile * n_conv
        right = lax.rem(index + 1, total)
        left = lax.rem(index + total - 1, total)
        right_id = (right // n_conv, lax.rem(right, n_conv))
        left_id = (left // n_conv, lax.rem(left, n_conv))

        def peer(d):
            return (tile, lax.rem(me + d, n_conv))

        loads = [
            pltpu.make_async_copy(edges, eg, load_sem.at[0]),
            pltpu.make_async_copy(field.at[:, pl.ds(columns - rim, rim)], xf.at[:, pl.ds(columns - rim, rim)], load_sem.at[1]),
            pltpu.make_async_copy(field.at[:, pl.ds(0, rim)], xf.at[:, pl.ds(0, rim)], load_sem.at[2]),
            pltpu.make_async_copy(owner, ow, load_sem.at[3]),
            pltpu.make_async_copy(interp, ib, load_sem.at[4]),
            pltpu.make_async_copy(
                field.at[:, pl.ds(rim, columns - 2 * rim)], xf.at[:, pl.ds(rim, columns - 2 * rim)], load_sem.at[5]
            ),
            pltpu.make_async_copy(conv, wb, load_sem.at[6]),
            pltpu.make_async_copy(shift, sh, load_sem.at[7]),
        ]
        for load in loads:
            load.start()

        def tell(semaphore, target):
            pl.semaphore_signal(semaphore, inc=1, device_id=target, device_id_type=MESH)

        barrier = pltpu.get_barrier_semaphore()
        tell(barrier, peer(n_conv - 1))
        tell(barrier, left_id)
        pl.semaphore_wait(barrier, 2)
        tell(near.at[0], peer(1))
        tell(near.at[1], right_id)

        for i in range(3):
            loads[i].wait()
        down = lax.broadcasted_iota(jnp.int32, (rim, rim), 0)
        pick_left = (down == eg[0:1, :]).astype(F32).astype(BF16)
        pick_right = (down + (columns - rim) == eg[1:2, :]).astype(F32).astype(BF16)
        edge_cols = (slice(columns - rim, columns), slice(0, rim))
        for side, pick in ((0, pick_right), (1, pick_left)):
            cells = xf[:, edge_cols[side]].astype(BF16)
            xb[:, edge_cols[side]] = cells
            rims[side] = mm(cells, pick).astype(BF16).reshape(halves, half, rim)

        def halo_copy(side, h):
            return pltpu.make_async_remote_copy(
                src_ref=rims.at[side, h], dst_ref=halo.at[side, h],
                send_sem=halo_send.at[side], recv_sem=halo_recv.at[side, h],
                device_id=(right_id, left_id)[side], device_id_type=MESH,
            )

        for h in range(halves):
            halo_copy(0, h).start()
        pl.semaphore_wait(near.at[0], 1)
        tell(up.at[0], peer(1))
        tell(down_sem.at[0], peer(n_conv - 1))

        @pl.when(me > 0)
        def _():
            pl.semaphore_wait(near.at[1], 1)
            for h in range(halves):
                halo_copy(1, h).start()

        def widen(step, reach):
            pl.semaphore_wait(up.at[step], 1)
            pl.semaphore_wait(down_sem.at[step], 1)
            if reach < n_conv // 2:
                tell(up.at[step + 1], peer(reach))
                tell(down_sem.at[step + 1], peer(n_conv - reach))

        loads[3].wait()
        owners = ow[...]
        named = (lax.broadcasted_iota(jnp.int32, (n_conv, points), 0) == owners).astype(F32)
        earlier = (
            lax.broadcasted_iota(jnp.int32, (points, points), 0) < lax.broadcasted_iota(jnp.int32, (points, points), 1)
        ).astype(F32).astype(BF16)
        before = mm(named.astype(BF16), earlier)
        rank = jnp.sum(before * named, axis=0, keepdims=True)
        slot = owners.astype(F32) * cap + rank
        pt[...] = (lax.broadcasted_iota(jnp.int32, (slots, points), 0).astype(F32) == slot).astype(F32).astype(BF16)
        widen(0, 2)
        loads[4].wait()
        extended = columns + 2 * rim
        for start in range(0, extended, 256):
            if start == 512:
                widen(1, 4)
            qt[:, start:start + 256] = mm(pt[...], ib[start:start + 256, :], NT).astype(BF16)
        loads[5].wait()
        xb[:, rim:columns - rim] = xf[:, rim:columns - rim].astype(BF16)
        for h in range(halves):
            mid[h] = mm(qt[:, rim:rim + columns], xb[h * half:(h + 1) * half, :], NT)

        widen(2, 8)

        @pl.when(me == 0)
        def _():
            pl.semaphore_wait(near.at[1], 1)
            for h in range(halves):
                halo_copy(1, h).start()

        g_t = (g_t0, g_t1)
        inc = (inc_t.at[0], inc_t.at[1])

        def exchange(h, src, dst, send, recv):
            mine = pl.ds(pl.multiple_of(me * cap, cap), cap)
            for d in offsets:
                to = lax.rem(me + d, n_conv)
                pltpu.make_async_remote_copy(
                    src_ref=src.at[h, pl.ds(pl.multiple_of(to * cap, cap), cap)],
                    dst_ref=dst.at[mine],
                    send_sem=send.at[h], recv_sem=recv.at[h],
                    device_id=peer(d), device_id_type=MESH,
                ).start()
            dst[mine, :] = src[h, mine, :]

        def exchanged(h, src, dst, send, recv):
            others = pl.ds(0, slots - cap)
            return pltpu.make_async_remote_copy(
                src_ref=src.at[h, others], dst_ref=dst.at[others],
                send_sem=send.at[h], recv_sem=recv.at[h],
                device_id=peer(1), device_id_type=MESH,
            )

        for h in range(halves):
            halo_copy(0, h).wait_recv()
            halo_copy(1, h).wait_recv()
            sub = mid[h] + mm(qt[:, 0:rim], halo[0, h], NT) + mm(qt[:, rim + columns:], halo[1, h], NT)
            out_t[h] = sub.astype(BF16)
            exchange(h, out_t, g_t[h], go_send, go_recv)

        loads[6].wait()
        loads[7].wait()
        for j in range(blocks):
            for c in range(bands):
                wt[j, :, c * block_points:(c + 1) * block_points] = wb[j, c].T

        for h in range(halves):
            exchanged(h, out_t, g_t[h], go_send, go_recv).wait_recv()
            pieces = [g_t[h][s * block_points:(s + 1) * block_points, :] for s in range(blocks)]
            sums = [None] * blocks
            for j in range(blocks):
                sources = [lax.rem(sh[j, c] + j, blocks) for c in range(bands)]
                picked = jnp.concatenate([choose(pieces, s) for s in sources], axis=0)
                forward = mm(wt[j], picked).astype(BF16)
                for c in range(bands):
                    term = mm(wb[j, c], forward)
                    for s in range(blocks):
                        part = term * (sources[c] == s).astype(F32)
                        sums[s] = part if sums[s] is None else sums[s] + part
            for s in range(blocks):
                adj_t[h, s * block_points:(s + 1) * block_points] = sums[s].astype(BF16)
            exchange(h, adj_t, inc[h], back_send, back_recv)

        edge_copies = []
        for h in range(halves):
            exchanged(h, adj_t, inc[h], back_send, back_recv).wait_recv()
            came = inc_t[h].T
            edge_out[0, h] = mm(came, qt[:, rim + columns:]).astype(BF16)
            edge_out[1, h] = mm(came, qt[:, 0:rim]).astype(BF16)
            for side, target in ((0, right_id), (1, left_id)):
                copy = pltpu.make_async_remote_copy(
                    src_ref=edge_out.at[side, h], dst_ref=edge_in.at[side, h],
                    send_sem=edge_send.at[side], recv_sem=edge_recv.at[side, h],
                    device_id=target, device_id_type=MESH,
                )
                copy.start()
                edge_copies.append(copy)
            out[h * half:(h + 1) * half, :] = mm(came, qt[:, rim:rim + columns])
        for h in range(halves):
            span = slice(h * half, (h + 1) * half)
            edge_copies[2 * h].wait_recv()
            edge_copies[2 * h + 1].wait_recv()
            out[span, 0:rim] += mm(edge_in[0, h], pick_left, NT)
            out[span, columns - rim:columns] += mm(edge_in[1, h], pick_right, NT)
        for side in range(2):
            for src, dst, send, recv in ((rims, halo, halo_send, halo_recv), (edge_out, edge_in, edge_send, edge_recv)):
                pltpu.make_async_remote_copy(
                    src_ref=src.at[side], dst_ref=dst.at[side], send_sem=send.at[side], recv_sem=recv.at[side, 0],
                    device_id=right_id, device_id_type=MESH,
                ).wait_send()
        for h in range(halves):
            exchanged(h, out_t, g_t[h], go_send, go_recv).wait_send()
            exchanged(h, adj_t, inc[h], back_send, back_recv).wait_send()

    return kernel


def solution(mesh):
    n_tile, n_conv = mesh.shape["tile"], mesh.shape["conv"]

    def on_device(field, interp, conv_blocks, band_shift, owner, edge_index):
        rows, columns = field.shape
        rim = edge_index.shape[1]
        extended, points = interp.shape
        blocks, bands, block_points, _ = conv_blocks.shape
        slots = blocks * block_points
        half, halves = 128, rows // 128
        body = make_kernel(n_tile, n_conv, rows, columns, rim, points, blocks, bands, block_points)
        sides = (2, halves, half, rim)
        cells = (halves, slots, half)
        operands = [
            pltpu.with_memory_space_constraint(x, pltpu.HBM)
            for x in (field, interp, conv_blocks, band_shift, owner.reshape(1, points), edge_index)
        ]
        return pl.pallas_call(
            body,
            out_shape=jax.ShapeDtypeStruct((rows, columns), F32),
            in_specs=[pl.BlockSpec(memory_space=pltpu.HBM)] * 6,
            out_specs=pl.BlockSpec(memory_space=pltpu.VMEM),
            scratch_shapes=[
                pltpu.VMEM((rows, columns), F32),
                pltpu.VMEM((extended, points), BF16),
                pltpu.VMEM((blocks, bands, block_points, block_points), BF16),
                pltpu.SMEM((blocks, bands), jnp.int32),
                pltpu.VMEM((1, points), jnp.int32),
                pltpu.VMEM((2, rim), jnp.int32),
                pltpu.VMEM(sides, BF16),
                pltpu.VMEM(sides, BF16),
                pltpu.VMEM((slots, points), BF16),
                pltpu.VMEM((slots, extended), BF16),
                pltpu.VMEM((rows, columns), BF16),
                pltpu.VMEM((halves, slots, half), F32),
                pltpu.VMEM(cells, BF16),
                pltpu.VMEM(cells[1:], BF16),
                pltpu.VMEM(cells[1:], BF16),
                pltpu.VMEM(cells, BF16),
                pltpu.VMEM(cells, BF16),
                pltpu.VMEM(sides, BF16),
                pltpu.VMEM(sides, BF16),
                pltpu.VMEM((blocks, block_points, bands * block_points), BF16),
                pltpu.SemaphoreType.DMA((8,)),
                pltpu.SemaphoreType.DMA((2,)),
                pltpu.SemaphoreType.DMA((2, halves)),
                pltpu.SemaphoreType.DMA((halves,)),
                pltpu.SemaphoreType.DMA((halves,)),
                pltpu.SemaphoreType.DMA((halves,)),
                pltpu.SemaphoreType.DMA((halves,)),
                pltpu.SemaphoreType.DMA((2,)),
                pltpu.SemaphoreType.DMA((2, halves)),
                pltpu.SemaphoreType.REGULAR((2,)),
                pltpu.SemaphoreType.REGULAR((3,)),
                pltpu.SemaphoreType.REGULAR((3,)),
            ],
            compiler_params=pltpu.CompilerParams(
                collective_id=0, has_side_effects=True, vmem_limit_bytes=24 * 1024 * 1024
            ),
        )(*operands)

    return jax.shard_map(
        on_device,
        mesh=mesh,
        in_specs=(
            P(None, ("tile", "conv")),
            P(("tile", "conv"), None),
            P(("tile", "conv"), None, None, None),
            P(("tile", "conv"), None),
            P(("tile", "conv"), None),
            P(("tile", "conv"), None),
        ),
        out_specs=P(None, ("tile", "conv")),
        check_vma=False,
    )
```

```python
import jax
import jax.numpy as jnp
from jax import lax
from jax.experimental import pallas as pl
from jax.experimental.pallas import tpu as pltpu
from jax.sharding import PartitionSpec as P

MESH = pl.DeviceIdType.MESH
F32 = jnp.float32
BF16 = jnp.bfloat16
NT = (((1,), (1,)), ((), ()))
NN = (((1,), (0,)), ((), ()))


def mm(a, b, dims=NN):
    return lax.dot_general(a, b, dims, preferred_element_type=F32)


def choose(pieces, source):
    chosen = pieces[0]
    for s in range(1, len(pieces)):
        chosen = jnp.where(source == s, pieces[s], chosen)
    return chosen


def make_kernel(n_tile, n_conv, rows, columns, rim, points, blocks, bands, block_points):
    slots = blocks * block_points
    cap = slots // n_conv
    half = 128
    halves = rows // half
    offsets = sorted(range(1, n_conv), key=lambda d: (-min(d, n_conv - d), d))

    def kernel(
        field, interp, conv, shift, owner, edges, out,
        xf, ib, wb, sh, ow, eg, rims, halo, pt, qt, xb, mid, out_t, g_t0, g_t1, adj_t, inc_t, edge_out, edge_in, wt,
        load_sem, halo_send, halo_recv, go_send, go_recv, back_send, back_recv, edge_send, edge_recv,
        near, up, down_sem,
    ):
        tile = lax.axis_index("tile")
        me = lax.axis_index("conv")
        index = tile * n_conv + me
        total = n_tile * n_conv
        right = lax.rem(index + 1, total)
        left = lax.rem(index + total - 1, total)
        right_id = (right // n_conv, lax.rem(right, n_conv))
        left_id = (left // n_conv, lax.rem(left, n_conv))

        def peer(d):
            return (tile, lax.rem(me + d, n_conv))

        loads = [
            pltpu.make_async_copy(edges, eg, load_sem.at[0]),
            pltpu.make_async_copy(field.at[:, pl.ds(columns - rim, rim)], xf.at[:, pl.ds(columns - rim, rim)], load_sem.at[1]),
            pltpu.make_async_copy(field.at[:, pl.ds(0, rim)], xf.at[:, pl.ds(0, rim)], load_sem.at[2]),
            pltpu.make_async_copy(owner, ow, load_sem.at[3]),
            pltpu.make_async_copy(interp, ib, load_sem.at[4]),
            pltpu.make_async_copy(
                field.at[:, pl.ds(rim, columns - 2 * rim)], xf.at[:, pl.ds(rim, columns - 2 * rim)], load_sem.at[5]
            ),
            pltpu.make_async_copy(conv, wb, load_sem.at[6]),
            pltpu.make_async_copy(shift, sh, load_sem.at[7]),
        ]
        for load in loads[:4]:
            load.start()

        def tell(semaphore, target):
            pl.semaphore_signal(semaphore, inc=1, device_id=target, device_id_type=MESH)

        barrier = pltpu.get_barrier_semaphore()
        tell(barrier, peer(n_conv - 1))
        tell(barrier, left_id)
        pl.semaphore_wait(barrier, 2)
        tell(near.at[0], peer(1))
        tell(near.at[1], right_id)

        loads[0].wait()
        loads[1].wait()
        for load in loads[4:]:
            load.start()
        down = lax.broadcasted_iota(jnp.int32, (rim, rim), 0)
        pick_left = (down == eg[0:1, :]).astype(F32).astype(BF16)
        pick_right = (down + (columns - rim) == eg[1:2, :]).astype(F32).astype(BF16)
        edge_cols = (slice(columns - rim, columns), slice(0, rim))

        def halo_copy(side, h):
            return pltpu.make_async_remote_copy(
                src_ref=rims.at[side, h], dst_ref=halo.at[side, h],
                send_sem=halo_send.at[side], recv_sem=halo_recv.at[side, h],
                device_id=(right_id, left_id)[side], device_id_type=MESH,
            )

        def fill_rim(side, pick):
            cells = xf[:, edge_cols[side]].astype(BF16)
            rims[side] = mm(cells, pick).astype(BF16).reshape(halves, half, rim)
            xb[:, edge_cols[side]] = cells

        fill_rim(0, pick_right)
        for h in range(halves):
            halo_copy(0, h).start()
        loads[2].wait()
        fill_rim(1, pick_left)
        pl.semaphore_wait(near.at[0], 1)
        tell(up.at[0], peer(1))
        tell(down_sem.at[0], peer(n_conv - 1))

        @pl.when(me > 0)
        def _():
            pl.semaphore_wait(near.at[1], 1)
            for h in range(halves):
                halo_copy(1, h).start()

        def widen(step, reach):
            pl.semaphore_wait(up.at[step], 1)
            pl.semaphore_wait(down_sem.at[step], 1)
            if reach < n_conv // 2:
                tell(up.at[step + 1], peer(reach))
                tell(down_sem.at[step + 1], peer(n_conv - reach))

        loads[3].wait()
        owners = ow[...]
        named = (lax.broadcasted_iota(jnp.int32, (n_conv, points), 0) == owners).astype(F32)
        earlier = (
            lax.broadcasted_iota(jnp.int32, (points, points), 0) < lax.broadcasted_iota(jnp.int32, (points, points), 1)
        ).astype(F32).astype(BF16)
        before = mm(named.astype(BF16), earlier)
        rank = jnp.sum(before * named, axis=0, keepdims=True)
        slot = owners.astype(F32) * cap + rank
        pt[...] = (lax.broadcasted_iota(jnp.int32, (slots, points), 0).astype(F32) == slot).astype(F32).astype(BF16)
        widen(0, 2)
        loads[4].wait()
        extended = columns + 2 * rim
        for start in range(0, extended, 256):
            if start == 512:
                widen(1, 4)
            qt[:, start:start + 256] = mm(pt[...], ib[start:start + 256, :], NT).astype(BF16)
        loads[5].wait()
        xb[:, rim:columns - rim] = xf[:, rim:columns - rim].astype(BF16)
        for h in range(halves):
            mid[h] = mm(qt[:, rim:rim + columns], xb[h * half:(h + 1) * half, :], NT)

        widen(2, 8)

        @pl.when(me == 0)
        def _():
            pl.semaphore_wait(near.at[1], 1)
            for h in range(halves):
                halo_copy(1, h).start()

        g_t = (g_t0, g_t1)
        inc = (inc_t.at[0], inc_t.at[1])

        def exchange(h, src, dst, send, recv):
            mine = pl.ds(pl.multiple_of(me * cap, cap), cap)
            for d in offsets:
                to = lax.rem(me + d, n_conv)
                pltpu.make_async_remote_copy(
                    src_ref=src.at[h, pl.ds(pl.multiple_of(to * cap, cap), cap)],
                    dst_ref=dst.at[mine],
                    send_sem=send.at[h], recv_sem=recv.at[h],
                    device_id=peer(d), device_id_type=MESH,
                ).start()
            dst[mine, :] = src[h, mine, :]

        def exchanged(h, src, dst, send, recv):
            others = pl.ds(0, slots - cap)
            return pltpu.make_async_remote_copy(
                src_ref=src.at[h, others], dst_ref=dst.at[others],
                send_sem=send.at[h], recv_sem=recv.at[h],
                device_id=peer(1), device_id_type=MESH,
            )

        for h in range(halves):
            halo_copy(0, h).wait_recv()
            halo_copy(1, h).wait_recv()
            sub = mid[h] + mm(qt[:, 0:rim], halo[0, h], NT) + mm(qt[:, rim + columns:], halo[1, h], NT)
            out_t[h] = sub.astype(BF16)
            exchange(h, out_t, g_t[h], go_send, go_recv)

        loads[6].wait()
        loads[7].wait()
        for j in range(blocks):
            for c in range(bands):
                wt[j, :, c * block_points:(c + 1) * block_points] = wb[j, c].T

        for h in range(halves):
            exchanged(h, out_t, g_t[h], go_send, go_recv).wait_recv()
            pieces = [g_t[h][s * block_points:(s + 1) * block_points, :] for s in range(blocks)]
            sums = [None] * blocks
            for j in range(blocks):
                sources = [lax.rem(sh[j, c] + j, blocks) for c in range(bands)]
                picked = jnp.concatenate([choose(pieces, s) for s in sources], axis=0)
                forward = mm(wt[j], picked).astype(BF16)
                for c in range(bands):
                    term = mm(wb[j, c], forward)
                    for s in range(blocks):
                        part = term * (sources[c] == s).astype(F32)
                        sums[s] = part if sums[s] is None else sums[s] + part
            for s in range(blocks):
                adj_t[h, s * block_points:(s + 1) * block_points] = sums[s].astype(BF16)
            exchange(h, adj_t, inc[h], back_send, back_recv)

        edge_copies = []
        for h in range(halves):
            exchanged(h, adj_t, inc[h], back_send, back_recv).wait_recv()
            came = inc_t[h].T
            edge_out[0, h] = mm(came, qt[:, rim + columns:]).astype(BF16)
            edge_out[1, h] = mm(came, qt[:, 0:rim]).astype(BF16)
            for side, target in ((0, right_id), (1, left_id)):
                copy = pltpu.make_async_remote_copy(
                    src_ref=edge_out.at[side, h], dst_ref=edge_in.at[side, h],
                    send_sem=edge_send.at[side], recv_sem=edge_recv.at[side, h],
                    device_id=target, device_id_type=MESH,
                )
                copy.start()
                edge_copies.append(copy)
            out[h * half:(h + 1) * half, :] = mm(came, qt[:, rim:rim + columns])
        for h in range(halves):
            span = slice(h * half, (h + 1) * half)
            edge_copies[2 * h].wait_recv()
            edge_copies[2 * h + 1].wait_recv()
            out[span, 0:rim] += mm(edge_in[0, h], pick_left, NT)
            out[span, columns - rim:columns] += mm(edge_in[1, h], pick_right, NT)
        for side in range(2):
            for src, dst, send, recv in ((rims, halo, halo_send, halo_recv), (edge_out, edge_in, edge_send, edge_recv)):
                pltpu.make_async_remote_copy(
                    src_ref=src.at[side], dst_ref=dst.at[side], send_sem=send.at[side], recv_sem=recv.at[side, 0],
                    device_id=right_id, device_id_type=MESH,
                ).wait_send()
        for h in range(halves):
            exchanged(h, out_t, g_t[h], go_send, go_recv).wait_send()
            exchanged(h, adj_t, inc[h], back_send, back_recv).wait_send()

    return kernel


def solution(mesh):
    n_tile, n_conv = mesh.shape["tile"], mesh.shape["conv"]

    def on_device(field, interp, conv_blocks, band_shift, owner, edge_index):
        rows, columns = field.shape
        rim = edge_index.shape[1]
        extended, points = interp.shape
        blocks, bands, block_points, _ = conv_blocks.shape
        slots = blocks * block_points
        half, halves = 128, rows // 128
        body = make_kernel(n_tile, n_conv, rows, columns, rim, points, blocks, bands, block_points)
        sides = (2, halves, half, rim)
        cells = (halves, slots, half)
        operands = [
            pltpu.with_memory_space_constraint(x, pltpu.HBM)
            for x in (field, interp, conv_blocks, band_shift, owner.reshape(1, points), edge_index)
        ]
        return pl.pallas_call(
            body,
            out_shape=jax.ShapeDtypeStruct((rows, columns), F32),
            in_specs=[pl.BlockSpec(memory_space=pltpu.HBM)] * 6,
            out_specs=pl.BlockSpec(memory_space=pltpu.VMEM),
            scratch_shapes=[
                pltpu.VMEM((rows, columns), F32),
                pltpu.VMEM((extended, points), BF16),
                pltpu.VMEM((blocks, bands, block_points, block_points), BF16),
                pltpu.SMEM((blocks, bands), jnp.int32),
                pltpu.VMEM((1, points), jnp.int32),
                pltpu.VMEM((2, rim), jnp.int32),
                pltpu.VMEM(sides, BF16),
                pltpu.VMEM(sides, BF16),
                pltpu.VMEM((slots, points), BF16),
                pltpu.VMEM((slots, extended), BF16),
                pltpu.VMEM((rows, columns), BF16),
                pltpu.VMEM((halves, slots, half), F32),
                pltpu.VMEM(cells, BF16),
                pltpu.VMEM(cells[1:], BF16),
                pltpu.VMEM(cells[1:], BF16),
                pltpu.VMEM(cells, BF16),
                pltpu.VMEM(cells, BF16),
                pltpu.VMEM(sides, BF16),
                pltpu.VMEM(sides, BF16),
                pltpu.VMEM((blocks, block_points, bands * block_points), BF16),
                pltpu.SemaphoreType.DMA((8,)),
                pltpu.SemaphoreType.DMA((2,)),
                pltpu.SemaphoreType.DMA((2, halves)),
                pltpu.SemaphoreType.DMA((halves,)),
                pltpu.SemaphoreType.DMA((halves,)),
                pltpu.SemaphoreType.DMA((halves,)),
                pltpu.SemaphoreType.DMA((halves,)),
                pltpu.SemaphoreType.DMA((2,)),
                pltpu.SemaphoreType.DMA((2, halves)),
                pltpu.SemaphoreType.REGULAR((2,)),
                pltpu.SemaphoreType.REGULAR((3,)),
                pltpu.SemaphoreType.REGULAR((3,)),
            ],
            compiler_params=pltpu.CompilerParams(
                collective_id=0, has_side_effects=True, vmem_limit_bytes=24 * 1024 * 1024
            ),
        )(*operands)

    return jax.shard_map(
        on_device,
        mesh=mesh,
        in_specs=(
            P(None, ("tile", "conv")),
            P(("tile", "conv"), None),
            P(("tile", "conv"), None, None, None),
            P(("tile", "conv"), None),
            P(("tile", "conv"), None),
            P(("tile", "conv"), None),
        ),
        out_specs=P(None, ("tile", "conv")),
        check_vma=False,
    )
```

```python
import jax
import jax.numpy as jnp
from jax import lax
from jax.experimental import pallas as pl
from jax.experimental.pallas import tpu as pltpu
from jax.sharding import PartitionSpec as P

MESH = pl.DeviceIdType.MESH
F32 = jnp.float32
BF16 = jnp.bfloat16
NT = (((1,), (1,)), ((), ()))
NN = (((1,), (0,)), ((), ()))


def mm(a, b, dims=NN):
    return lax.dot_general(a, b, dims, preferred_element_type=F32)


def choose(pieces, source):
    chosen = pieces[0]
    for s in range(1, len(pieces)):
        chosen = jnp.where(source == s, pieces[s], chosen)
    return chosen


def make_kernel(n_tile, n_conv, rows, columns, rim, points, blocks, bands, block_points):
    slots = blocks * block_points
    cap = slots // n_conv
    half = 128
    halves = rows // half
    offsets = sorted(range(1, n_conv), key=lambda d: (-min(d, n_conv - d), d))

    far = 9

    def kernel(
        field, interp, conv, shift, owner, edges, out,
        xf, ib, wb, sh, ow, eg, rims, halo, pt, qt, xb, mid, out_t, g_t0, g_t1, adj_t, inc_t, edge_out, edge_in, wt,
        load_sem, halo_send, halo_recv, go_send, go_recv, back_send, back_recv, edge_send, edge_recv,
        near, up, down_sem,
    ):
        tile = lax.axis_index("tile")
        me = lax.axis_index("conv")
        index = tile * n_conv + me
        total = n_tile * n_conv
        right = lax.rem(index + 1, total)
        left = lax.rem(index + total - 1, total)
        right_id = (right // n_conv, lax.rem(right, n_conv))
        left_id = (left // n_conv, lax.rem(left, n_conv))

        def peer(d):
            return (tile, lax.rem(me + d, n_conv))

        loads = [
            pltpu.make_async_copy(edges, eg, load_sem.at[0]),
            pltpu.make_async_copy(field.at[:, pl.ds(columns - rim, rim)], xf.at[:, pl.ds(columns - rim, rim)], load_sem.at[1]),
            pltpu.make_async_copy(field.at[:, pl.ds(0, rim)], xf.at[:, pl.ds(0, rim)], load_sem.at[2]),
            pltpu.make_async_copy(owner, ow, load_sem.at[3]),
            pltpu.make_async_copy(interp, ib, load_sem.at[4]),
            pltpu.make_async_copy(
                field.at[:, pl.ds(rim, columns - 2 * rim)], xf.at[:, pl.ds(rim, columns - 2 * rim)], load_sem.at[5]
            ),
            pltpu.make_async_copy(conv, wb, load_sem.at[6]),
            pltpu.make_async_copy(shift, sh, load_sem.at[7]),
        ]
        for load in loads[:4]:
            load.start()

        def tell(semaphore, target):
            pl.semaphore_signal(semaphore, inc=1, device_id=target, device_id_type=MESH)

        barrier = pltpu.get_barrier_semaphore()
        tell(barrier, peer(n_conv - 1))
        tell(barrier, left_id)
        pl.semaphore_wait(barrier, 2)
        tell(near.at[0], peer(1))
        tell(near.at[1], right_id)

        loads[0].wait()
        loads[1].wait()
        for load in loads[4:]:
            load.start()
        down = lax.broadcasted_iota(jnp.int32, (rim, rim), 0)
        pick_left = (down == eg[0:1, :]).astype(F32).astype(BF16)
        pick_right = (down + (columns - rim) == eg[1:2, :]).astype(F32).astype(BF16)
        edge_cols = (slice(columns - rim, columns), slice(0, rim))

        def halo_copy(side, h):
            return pltpu.make_async_remote_copy(
                src_ref=rims.at[side, h], dst_ref=halo.at[side, h],
                send_sem=halo_send.at[side], recv_sem=halo_recv.at[side, h],
                device_id=(right_id, left_id)[side], device_id_type=MESH,
            )

        def fill_rim(side, pick):
            cells = xf[:, edge_cols[side]].astype(BF16)
            rims[side] = mm(cells, pick).astype(BF16).reshape(halves, half, rim)
            xb[:, edge_cols[side]] = cells

        fill_rim(0, pick_right)
        for h in range(halves):
            halo_copy(0, h).start()
        loads[2].wait()
        fill_rim(1, pick_left)
        pl.semaphore_wait(near.at[0], 1)
        tell(up.at[0], peer(1))
        tell(down_sem.at[0], peer(n_conv - 1))

        @pl.when(me > 0)
        def _():
            pl.semaphore_wait(near.at[1], 1)
            for h in range(halves):
                halo_copy(1, h).start()

        def widen(step, reach):
            pl.semaphore_wait(up.at[step], 1)
            pl.semaphore_wait(down_sem.at[step], 1)
            if reach < n_conv // 2:
                tell(up.at[step + 1], peer(reach))
                tell(down_sem.at[step + 1], peer(n_conv - reach))

        loads[3].wait()
        owners = ow[...]
        named = (lax.broadcasted_iota(jnp.int32, (n_conv, points), 0) == owners).astype(F32)
        earlier = (
            lax.broadcasted_iota(jnp.int32, (points, points), 0) < lax.broadcasted_iota(jnp.int32, (points, points), 1)
        ).astype(F32).astype(BF16)
        before = mm(named.astype(BF16), earlier)
        rank = jnp.sum(before * named, axis=0, keepdims=True)
        slot = owners.astype(F32) * cap + rank
        pt[...] = (lax.broadcasted_iota(jnp.int32, (slots, points), 0).astype(F32) == slot).astype(F32).astype(BF16)
        widen(0, 2)
        loads[4].wait()
        extended = columns + 2 * rim
        for start in range(0, extended, 256):
            if start == 512:
                widen(1, 4)
            qt[:, start:start + 256] = mm(pt[...], ib[start:start + 256, :], NT).astype(BF16)
        loads[5].wait()
        xb[:, rim:columns - rim] = xf[:, rim:columns - rim].astype(BF16)
        for h in range(halves):
            mid[h] = mm(qt[:, rim:rim + columns], xb[h * half:(h + 1) * half, :], NT)

        widen(2, 8)

        @pl.when(me == 0)
        def _():
            pl.semaphore_wait(near.at[1], 1)
            for h in range(halves):
                halo_copy(1, h).start()

        g_t = (g_t0, g_t1)
        inc = (inc_t.at[0], inc_t.at[1])

        def exchange(h, src, dst, send, recv, steps):
            mine = pl.ds(pl.multiple_of(me * cap, cap), cap)
            for d in steps:
                to = lax.rem(me + d, n_conv)
                pltpu.make_async_remote_copy(
                    src_ref=src.at[h, pl.ds(pl.multiple_of(to * cap, cap), cap)],
                    dst_ref=dst.at[mine],
                    send_sem=send.at[h], recv_sem=recv.at[h],
                    device_id=peer(d), device_id_type=MESH,
                ).start()
            if len(steps) > 1 and steps[0] == offsets[0]:
                dst[mine, :] = src[h, mine, :]

        def exchanged(h, src, dst, send, recv):
            others = pl.ds(0, slots - cap)
            return pltpu.make_async_remote_copy(
                src_ref=src.at[h, others], dst_ref=dst.at[others],
                send_sem=send.at[h], recv_sem=recv.at[h],
                device_id=peer(1), device_id_type=MESH,
            )

        for h in range(halves):
            halo_copy(0, h).wait_recv()
            halo_copy(1, h).wait_recv()
            sub = mid[h] + mm(qt[:, 0:rim], halo[0, h], NT) + mm(qt[:, rim + columns:], halo[1, h], NT)
            out_t[h] = sub.astype(BF16)
            exchange(h, out_t, g_t[h], go_send, go_recv, offsets)

        loads[6].wait()
        loads[7].wait()
        for j in range(blocks):
            for c in range(bands):
                wt[j, :, c * block_points:(c + 1) * block_points] = wb[j, c].T

        for h in range(halves):
            exchanged(h, out_t, g_t[h], go_send, go_recv).wait_recv()
            pieces = [g_t[h][s * block_points:(s + 1) * block_points, :] for s in range(blocks)]
            sums = [None] * blocks
            for j in range(blocks):
                sources = [lax.rem(sh[j, c] + j, blocks) for c in range(bands)]
                picked = jnp.concatenate([choose(pieces, s) for s in sources], axis=0)
                forward = mm(wt[j], picked).astype(BF16)
                for c in range(bands):
                    term = mm(wb[j, c], forward)
                    for s in range(blocks):
                        part = term * (sources[c] == s).astype(F32)
                        sums[s] = part if sums[s] is None else sums[s] + part
            for s in range(blocks):
                adj_t[h, s * block_points:(s + 1) * block_points] = sums[s].astype(BF16)
            exchange(h, adj_t, inc[h], back_send, back_recv, offsets[:far])
        for d in offsets[far:]:
            for h in range(halves):
                exchange(h, adj_t, inc[h], back_send, back_recv, [d])

        edge_copies = []
        for h in range(halves):
            exchanged(h, adj_t, inc[h], back_send, back_recv).wait_recv()
            came = inc_t[h].T
            edge_out[0, h] = mm(came, qt[:, rim + columns:]).astype(BF16)
            edge_out[1, h] = mm(came, qt[:, 0:rim]).astype(BF16)
            for side, target in ((0, right_id), (1, left_id)):
                copy = pltpu.make_async_remote_copy(
                    src_ref=edge_out.at[side, h], dst_ref=edge_in.at[side, h],
                    send_sem=edge_send.at[side], recv_sem=edge_recv.at[side, h],
                    device_id=target, device_id_type=MESH,
                )
                copy.start()
                edge_copies.append(copy)
            out[h * half:(h + 1) * half, :] = mm(came, qt[:, rim:rim + columns])
        for h in range(halves):
            span = slice(h * half, (h + 1) * half)
            edge_copies[2 * h].wait_recv()
            edge_copies[2 * h + 1].wait_recv()
            out[span, 0:rim] += mm(edge_in[0, h], pick_left, NT)
            out[span, columns - rim:columns] += mm(edge_in[1, h], pick_right, NT)
        for side in range(2):
            for src, dst, send, recv in ((rims, halo, halo_send, halo_recv), (edge_out, edge_in, edge_send, edge_recv)):
                pltpu.make_async_remote_copy(
                    src_ref=src.at[side], dst_ref=dst.at[side], send_sem=send.at[side], recv_sem=recv.at[side, 0],
                    device_id=right_id, device_id_type=MESH,
                ).wait_send()
        for h in range(halves):
            exchanged(h, out_t, g_t[h], go_send, go_recv).wait_send()
            exchanged(h, adj_t, inc[h], back_send, back_recv).wait_send()

    return kernel


def solution(mesh):
    n_tile, n_conv = mesh.shape["tile"], mesh.shape["conv"]

    def on_device(field, interp, conv_blocks, band_shift, owner, edge_index):
        rows, columns = field.shape
        rim = edge_index.shape[1]
        extended, points = interp.shape
        blocks, bands, block_points, _ = conv_blocks.shape
        slots = blocks * block_points
        half, halves = 128, rows // 128
        body = make_kernel(n_tile, n_conv, rows, columns, rim, points, blocks, bands, block_points)
        sides = (2, halves, half, rim)
        cells = (halves, slots, half)
        operands = [
            pltpu.with_memory_space_constraint(x, pltpu.HBM)
            for x in (field, interp, conv_blocks, band_shift, owner.reshape(1, points), edge_index)
        ]
        return pl.pallas_call(
            body,
            out_shape=jax.ShapeDtypeStruct((rows, columns), F32),
            in_specs=[pl.BlockSpec(memory_space=pltpu.HBM)] * 6,
            out_specs=pl.BlockSpec(memory_space=pltpu.VMEM),
            scratch_shapes=[
                pltpu.VMEM((rows, columns), F32),
                pltpu.VMEM((extended, points), BF16),
                pltpu.VMEM((blocks, bands, block_points, block_points), BF16),
                pltpu.SMEM((blocks, bands), jnp.int32),
                pltpu.VMEM((1, points), jnp.int32),
                pltpu.VMEM((2, rim), jnp.int32),
                pltpu.VMEM(sides, BF16),
                pltpu.VMEM(sides, BF16),
                pltpu.VMEM((slots, points), BF16),
                pltpu.VMEM((slots, extended), BF16),
                pltpu.VMEM((rows, columns), BF16),
                pltpu.VMEM((halves, slots, half), F32),
                pltpu.VMEM(cells, BF16),
                pltpu.VMEM(cells[1:], BF16),
                pltpu.VMEM(cells[1:], BF16),
                pltpu.VMEM(cells, BF16),
                pltpu.VMEM(cells, BF16),
                pltpu.VMEM(sides, BF16),
                pltpu.VMEM(sides, BF16),
                pltpu.VMEM((blocks, block_points, bands * block_points), BF16),
                pltpu.SemaphoreType.DMA((8,)),
                pltpu.SemaphoreType.DMA((2,)),
                pltpu.SemaphoreType.DMA((2, halves)),
                pltpu.SemaphoreType.DMA((halves,)),
                pltpu.SemaphoreType.DMA((halves,)),
                pltpu.SemaphoreType.DMA((halves,)),
                pltpu.SemaphoreType.DMA((halves,)),
                pltpu.SemaphoreType.DMA((2,)),
                pltpu.SemaphoreType.DMA((2, halves)),
                pltpu.SemaphoreType.REGULAR((2,)),
                pltpu.SemaphoreType.REGULAR((3,)),
                pltpu.SemaphoreType.REGULAR((3,)),
            ],
            compiler_params=pltpu.CompilerParams(
                collective_id=0, has_side_effects=True, vmem_limit_bytes=24 * 1024 * 1024
            ),
        )(*operands)

    return jax.shard_map(
        on_device,
        mesh=mesh,
        in_specs=(
            P(None, ("tile", "conv")),
            P(("tile", "conv"), None),
            P(("tile", "conv"), None, None, None),
            P(("tile", "conv"), None),
            P(("tile", "conv"), None),
            P(("tile", "conv"), None),
        ),
        out_specs=P(None, ("tile", "conv")),
        check_vma=False,
    )
```
